768 devices in a mesh: dp: 32 (over x, z_hi, core), mp: 24 (over z_lo, y).
Axes of the slice: x: 4, y: 8, z: 12 (z_hi: 4, z_lo: 3; z = z_hi * 3 + z_lo), core: 2. Of those that a mesh axis runs over, the one named last changes fastest.
Arguments:
- image_tokens: bfloat16 [3072, 32, 1152], P('dp'), may hold values from -6 to 6
- image_counts: int32 [32, 24], P('dp'), may hold values from 2 to 4, as said below
- image_ids: int32 [3072], P('dp'), may hold values from 0 to 767
- norm_gain: float32 [1152], replicated, may hold values from 0.1 to 1.9
- norm_bias: float32 [1152], replicated, may hold values from -3 to 3
- up_weight: bfloat16 [1152, 3072], P(None, 'mp'), may hold values from -0.1875 to 0.1875
- down_weight: bfloat16 [3072, 1152], P('mp'), may hold values from -0.109375 to 0.109375
- text_rows: bfloat16 [3072, 1152], P(('dp', 'mp')), may hold values from -6 to 6
- text_counts: int32 [768], P(('dp', 'mp')), may hold values from 2 to 4, as said below
- text_ids: int32 [3072], replicated, may hold values from 0 to 767
- logit_scale: float32 [1], replicated, may hold values from 30 to 45
- logit_bias: float32 [1], replicated, may hold values from -8 to -5.5
Outputs:
- text_grad: float32 [3072, 1152], P(('dp', 'mp'))
The draws below stay inside these ranges and needn't reach their ends.
Inputs may be any that keep to these rules, and one draw needn't show every extreme that they name: `image_counts`: entries count the valid rows among the 4 padded rows of one device's block; in every draw some block has all 4 rows valid. `text_counts`: entries count the valid rows among the 4 padded rows of one device's block; in every draw some block has all 4 rows valid.
All inputs are finite; a program needn't handle non-finite values.
Results may differ from the reference program's by a relative error of at most 0.02.
Values may be sent and summed in bfloat16 or wider, within the bound.
A program may use at most 32 MiB of HBM per device.

```python
import jax
import jax.numpy as jnp
from jax import lax

D = 1152
FF = 3072
ROWS_DEV = 4
PATCHES = 32
DATA_SHARDS = 32
WIDTH_SHARDS = 24
ROWS = 3072


def valid_counts(key, count_shape):
    counts = jax.random.randint(key, count_shape, ROWS_DEV // 2, ROWS_DEV + 1)
    flattened = counts.reshape(-1)
    chosen = jax.random.randint(jax.random.fold_in(key, 11), (), 0, flattened.shape[0])
    flattened = flattened.at[chosen].set(ROWS_DEV)
    return flattened.reshape(count_shape).astype(jnp.int32)


def draw_image_counts(key, part):
    return valid_counts(jax.random.fold_in(key, 1), (DATA_SHARDS, WIDTH_SHARDS))


def draw_text_counts(key, part):
    return valid_counts(jax.random.fold_in(key, 2), (DATA_SHARDS * WIDTH_SHARDS,))


def direction_table(key):
    return jax.random.normal(jax.random.fold_in(key, 7), (ROWS // 8, D), jnp.float32)


def draw_image_tokens(key, part):
    directions = direction_table(key)
    choose = jax.random.randint(jax.random.fold_in(key, 21), (ROWS,), 0, ROWS // 8)
    strength = jax.random.uniform(jax.random.fold_in(key, 22), (ROWS,), jnp.float32, 0.35, 0.7)
    jitter = jax.random.normal(jax.random.fold_in(key, 23), (ROWS, PATCHES, D), jnp.float32)
    centers = jnp.take(directions, choose, axis=0) * strength[:, None]
    values = jitter + centers[:, None, :]
    return jnp.clip(values, -6.0, 6.0).astype(jnp.bfloat16)


def draw_text_rows(key, part):
    directions = direction_table(key)
    choose = jax.random.randint(jax.random.fold_in(key, 31), (ROWS,), 0, ROWS // 8)
    strength = jax.random.uniform(jax.random.fold_in(key, 32), (ROWS,), jnp.float32, 0.15, 0.4)
    jitter = jax.random.normal(jax.random.fold_in(key, 33), (ROWS, D), jnp.float32)
    values = jitter + jnp.take(directions, choose, axis=0) * strength[:, None]
    return jnp.clip(values, -6.0, 6.0).astype(jnp.bfloat16)


def place_ends(values, rng, smallest, top_value):
    spot = [jax.random.randint(jax.random.fold_in(rng, axis), (), 0, length) for axis, length in enumerate(values.shape)]
    longest = values.shape.index(max(values.shape))
    neighbour = spot[:longest] + [(spot[longest] + 1) % values.shape[longest]] + spot[longest + 1:]
    return values.at[tuple(spot)].set(smallest).at[tuple(neighbour)].set(top_value)


def levels(rng, dims, shards, low, high):
    factor_of, own = 1.0, jax.random.fold_in(rng, 6)
    for position, shards_of in shards:
        heights = jnp.exp(jax.random.uniform(jax.random.fold_in(own, position), (shards_of,), jnp.float32, low / len(shards), high / len(shards)))
        factor_of = factor_of * jnp.repeat(heights, dims[position] // shards_of).reshape([-1 if axis == position else 1 for axis in range(len(dims))])
    return factor_of


def normal_values(own_key, extent, deviation, bound, cuts=(), held_as=jnp.bfloat16):
    values = deviation * jax.random.normal(own_key, extent, jnp.float32)
    if cuts:
        values = values * levels(own_key, extent, cuts, -0.22, 0.18)
    return jnp.clip(values, -bound, bound).astype(held_as)


def setup_inputs(seed: int = 0) -> dict:
    key_of = jax.random.split(jax.random.key(seed), 13)
    image_tokens = draw_image_tokens(jax.random.fold_in(key_of[12], 71), 0)
    image_counts = draw_image_counts(jax.random.fold_in(key_of[12], 71), 0)
    image_ids = place_ends(jax.random.randint(key_of[2], (ROWS,), 0, ROWS // 4), jax.random.fold_in(key_of[2], 1), 0, (ROWS // 4) - 1).astype(jnp.int32)
    norm_gain = jnp.clip(1.0 + 0.18 * jax.random.normal(key_of[3], (D,), jnp.float32), 0.1, 1.9)
    norm_bias = normal_values(key_of[4], (D,), 0.5, 3.0, (), jnp.float32)
    up_weight = normal_values(key_of[5], (D, FF), D ** -0.5, 0.1875, ((1, 24),))
    down_weight = normal_values(key_of[6], (FF, D), FF ** -0.5, 0.109375, ((0, 24),))
    text_rows = draw_text_rows(jax.random.fold_in(key_of[12], 71), 0)
    text_counts = draw_text_counts(jax.random.fold_in(key_of[12], 71), 0)
    text_ids = place_ends(jax.random.randint(key_of[9], (ROWS,), 0, ROWS // 4), jax.random.fold_in(key_of[9], 1), 0, (ROWS // 4) - 1).astype(jnp.int32)
    logit_scale = jnp.clip(jax.random.uniform(key_of[10], (1,), jnp.float32, 30.0, 45.0), 30.0, 45.0)
    logit_bias = jnp.clip(jax.random.uniform(key_of[11], (1,), jnp.float32, -8.0, -5.5), -8.0, -5.5)
    return dict(image_tokens=image_tokens, image_counts=image_counts, image_ids=image_ids, norm_gain=norm_gain, norm_bias=norm_bias, up_weight=up_weight, down_weight=down_weight, text_rows=text_rows, text_counts=text_counts, text_ids=text_ids, logit_scale=logit_scale, logit_bias=logit_bias)


norm_eps = 1e-06

def layer_norm(row_values, gain_row, shift_row):
    values = row_values.astype(jnp.float32)
    center = lax.optimization_barrier(jnp.mean(values, axis=-1, keepdims=True))
    spread = lax.optimization_barrier(jnp.mean(jnp.square(values - center), axis=-1, keepdims=True))
    return (values - center) * lax.rsqrt(spread + norm_eps) * gain_row + shift_row

def unit_rows(values):
    return values * lax.rsqrt(lax.optimization_barrier(jnp.sum(values * values, axis=-1, keepdims=True)) + norm_eps)

def pool_hidden(token_block, gain_row, shift_row, up_weight):
    normed = layer_norm(token_block, gain_row, shift_row).astype(jnp.bfloat16)
    hidden = jax.nn.gelu(jnp.dot(normed, up_weight, preferred_element_type=jnp.float32)).astype(jnp.bfloat16)
    return lax.optimization_barrier(jnp.mean(hidden.astype(jnp.float32), axis=1)).astype(jnp.bfloat16)

def pair_terms(text_block, block_ids, image_emb, image_ids, image_valid, logit_mul, logit_add):
    cosines = lax.dot_general(text_block, image_emb, (((1,), (1,)), ((), ())), preferred_element_type=jnp.float32)
    logits = logit_mul * cosines + logit_add
    sign_table = jnp.where(block_ids[:, None] == image_ids[None, :], 1.0, -1.0).astype(jnp.float32)
    margin = -sign_table * logits
    weights = (image_valid[None, :] * -sign_table * jax.nn.sigmoid(margin) * logit_mul).astype(jnp.bfloat16)
    return jnp.dot(weights, image_emb, preferred_element_type=jnp.float32)

def reference(image_tokens, image_counts, image_ids, norm_gain, norm_bias, up_weight, down_weight, text_rows, text_counts, text_ids, logit_scale, logit_bias):
    token_groups = image_tokens.reshape(ROWS // ROWS_DEV, ROWS_DEV, PATCHES, D)

    def one_group(token_block):
        return pool_hidden(token_block, norm_gain, norm_bias, up_weight)
    pooled_hidden = lax.map(one_group, token_groups).reshape(ROWS, FF)
    pooled_tokens = lax.optimization_barrier(jnp.mean(image_tokens.astype(jnp.float32), axis=1))
    tower_out = pooled_tokens + jnp.dot(pooled_hidden, down_weight, preferred_element_type=jnp.float32)
    image_emb = unit_rows(tower_out).astype(jnp.bfloat16)
    text_emb = unit_rows(text_rows.astype(jnp.float32)).astype(jnp.bfloat16)
    slot_index = jnp.arange(ROWS, dtype=jnp.int32) % ROWS_DEV
    image_valid = (slot_index < jnp.repeat(image_counts.reshape(-1), ROWS_DEV, total_repeat_length=ROWS)).astype(jnp.float32)
    text_valid = (slot_index < jnp.repeat(text_counts.reshape(-1), ROWS_DEV, total_repeat_length=ROWS)).astype(jnp.float32)
    text_block_rows = ROWS_DEV * WIDTH_SHARDS
    blocks = text_emb.reshape(ROWS // text_block_rows, text_block_rows, D)
    id_blocks = text_ids.reshape(ROWS // text_block_rows, text_block_rows)
    logit_mul = logit_scale[0]
    logit_add = logit_bias[0]

    def one_block(members):
        return pair_terms(members[0], members[1], image_emb, image_ids, image_valid, logit_mul, logit_add)
    grad_rows = lax.map(one_block, (blocks, id_blocks)).reshape(ROWS, D)
    return grad_rows * text_valid[:, None]
```

```python
import functools

import jax
import jax.numpy as jnp
from jax import lax
from jax.experimental import pallas as pl
from jax.experimental.pallas import tpu as pltpu
from jax.sharding import PartitionSpec as P

MESH = pl.DeviceIdType.MESH
EPS = 1e-06
F32 = jnp.float32
BF16 = jnp.bfloat16
GEOMETRY = (4, 4, 3, 8)


def await_bytes(ref, sem):
    pltpu.make_async_copy(ref, ref, sem).wait()


def unit_rows(values):
    return values * lax.rsqrt(jnp.sum(values * values, axis=-1, keepdims=True) + EPS)


def y_offset(step, ny):
    half = (step + 1) // 2
    return ny // 2 + half * (1 - 2 * (step % 2))


def kernel(
    geometry,
    tokens,
    counts,
    image_ids,
    gain,
    shift,
    w_up,
    w_down,
    text_rows,
    text_ids,
    scale,
    bias,
    out,
    x_buf,
    counts_v,
    ids_v,
    gain_v,
    shift_v,
    up_v,
    down_v,
    text_v,
    text_ids_s,
    scale_v,
    bias_v,
    w_aug,
    w_sum,
    w_shift,
    part_send,
    part_recv,
    own_part,
    emb_own,
    emb_peer,
    meta_own,
    meta_peer,
    text_all,
    rows_f32,
    grad_send,
    grad_recv,
    own_grad,
    in_sem,
    x_sem,
    part_send_sem,
    part_recv_sem,
    emb_send_sem,
    emb_recv_sem,
    pair_send_sem,
    pair_recv_sem,
    meta_send_sem,
    meta_recv_sem,
    text_send_sem,
    text_recv_sem,
    grad_send_sem,
    grad_recv_sem,
):
    nx, nzh, nzl, ny = geometry
    width = nzl * ny
    chips = nx * nzh
    rows, d = text_rows.shape
    patches = tokens.shape[1]
    units = w_up.shape[1]
    group = width * rows
    lanes = d // 128
    dp = lax.axis_index("dp")
    mp = lax.axis_index("mp")
    core = dp % 2
    my_x = dp // (2 * nzh)
    my_zh = (dp // 2) % nzh
    my_zl = mp // ny
    my_y = mp % ny
    partner = dp + 1 - 2 * core

    def mp_of(y_off, z_off):
        return ((my_zl + z_off) % nzl) * ny + (my_y + y_off) % ny

    def dp_of(x_off, z_off):
        return (((my_x + x_off) % nx) * nzh + (my_zh + z_off) % nzh) * 2 + core

    mp_partners = [
        (y_off, z_off)
        for y_off in [y_offset(s, ny) for s in range(ny)]
        for z_off in [(z + 1) % nzl for z in range(nzl)]
    ][:-1]
    z_order = sorted(range(nzh), key=lambda o: -min(o, nzh - o))
    x_order = sorted(range(nx), key=lambda o: -min(o, nx - o))
    dp_partners = [(x_off, z_off) for z_off in z_order for x_off in x_order][:-1]

    barrier = pltpu.get_barrier_semaphore()
    for y_off, z_off in mp_partners:
        pl.semaphore_signal(barrier, inc=1, device_id=(dp, mp_of(y_off, z_off)), device_id_type=MESH)
    for x_off, z_off in dp_partners:
        pl.semaphore_signal(barrier, inc=1, device_id=(dp_of(x_off, z_off), mp), device_id_type=MESH)
    pl.semaphore_signal(barrier, inc=1, device_id=(partner, mp), device_id_type=MESH)

    small = [
        (w_up, up_v),
        (gain, gain_v),
        (shift, shift_v),
        (w_down, down_v),
        (text_rows, text_v),
        (counts, counts_v),
        (image_ids, ids_v),
        (text_ids, text_ids_s),
        (scale, scale_v),
        (bias, bias_v),
    ]
    for index, (source, target) in enumerate(small[:3]):
        pltpu.make_async_copy(source, target, in_sem.at[index]).start()

    def load(step, z_off):
        start = mp_of(y_offset(step, ny), z_off) * rows
        pltpu.make_async_copy(
            tokens.at[pl.ds(start, rows)], x_buf.at[step, pl.ds(z_off * rows, rows)], x_sem.at[step]
        ).start()

    for step in range(ny):
        for z_off in range(nzl):
            load(step, z_off)
        if step == 0:
            for index, (source, target) in enumerate(small):
                if index >= 3:
                    pltpu.make_async_copy(source, target, in_sem.at[index]).start()

    for index in range(3):
        pltpu.make_async_copy(*small[index], in_sem.at[index]).wait()

    total = jnp.zeros((1, units), F32)
    moved = jnp.zeros((1, units), F32)
    for j in range(lanes):
        cut = pl.ds(j * 128, 128)
        block = up_v[cut, :].astype(F32)
        gain_column = jnp.transpose(jnp.broadcast_to(gain_v[:, cut], (128, 128)))[:, :1]
        shift_column = jnp.transpose(jnp.broadcast_to(shift_v[:, cut], (128, 128)))[:, :1]
        scaled = (block * gain_column).astype(BF16)
        w_aug[cut, pl.ds(0, units)] = scaled
        w_aug[cut, pl.ds(units, 128)] = jnp.ones((128, 128), BF16)
        total += jnp.sum(scaled.astype(F32), axis=0, keepdims=True)
        moved += jnp.sum(block * shift_column, axis=0, keepdims=True)
    w_sum[...] = total
    w_shift[...] = moved

    for index in range(3, len(small)):
        pltpu.make_async_copy(*small[index], in_sem.at[index]).wait()

    my_chip = dp // 2
    text_all[my_chip] = unit_rows(text_v[...].astype(F32)).astype(BF16)
    slot = lax.broadcasted_iota(jnp.int32, (width, group), 1)
    owner = lax.broadcasted_iota(jnp.int32, (width, group), 0)
    spread = jnp.where(slot // rows == owner, 1.0, 0.0).astype(BF16)
    row_counts = jnp.dot(
        jnp.broadcast_to(counts_v[...].astype(F32), (8, width)).astype(BF16),
        spread,
        preferred_element_type=F32,
    )[:1]
    place = (lax.broadcasted_iota(jnp.int32, (1, group), 1) % rows).astype(F32)
    meta_own[pl.ds(0, 1), pl.ds(0, group)] = ids_v[...].astype(F32)
    meta_own[pl.ds(1, 1), pl.ds(0, group)] = jnp.where(place < row_counts, 1.0, 0.0)

    pl.semaphore_wait(barrier, len(mp_partners) + len(dp_partners) + 1)

    meta_copy = pltpu.make_async_remote_copy(
        meta_own, meta_peer, meta_send_sem, meta_recv_sem, device_id=(partner, mp), device_id_type=MESH
    )
    meta_copy.start()
    for x_off, z_off in dp_partners:
        pltpu.make_async_remote_copy(
            text_all.at[my_chip],
            text_all.at[my_chip],
            text_send_sem,
            text_recv_sem,
            device_id=(dp_of(x_off, z_off), mp),
            device_id_type=MESH,
        ).start()

    def chunk(step, carry):
        await_bytes(x_buf.at[step], x_sem.at[step])
        images = nzl * rows
        count = images * patches
        x = x_buf[step].reshape(count, d)
        product = jnp.dot(x, w_aug[...], preferred_element_type=F32)
        mean = product[:, units:] * (1.0 / d)
        squares = jnp.zeros((count, 128), F32)
        for j in range(lanes):
            piece = x_buf[step, :, :, pl.ds(j * 128, 128)].reshape(count, 128).astype(F32) - mean
            squares += piece * piece
        spread_of = lax.rsqrt(jnp.sum(squares, axis=-1, keepdims=True) * (1.0 / d) + EPS)
        before = (product[:, :units] - mean * w_sum[...]) * spread_of + w_shift[...]
        hidden = jax.nn.gelu(before).astype(BF16).astype(F32)
        pooled = jnp.sum(hidden.reshape(images, patches, units), axis=1) * (1.0 / patches)
        part = jnp.dot(pooled.astype(BF16), down_v[...], preferred_element_type=F32)
        y_off = y_offset(step, ny)
        for z_off in [(z + 1) % nzl for z in range(nzl)]:
            term = part[z_off * rows : (z_off + 1) * rows]
            where_to = step * nzl + (z_off + nzl - 1) % nzl

            def send(term=term, where_to=where_to, z_off=z_off):
                part_send[where_to] = term.astype(BF16)
                pltpu.make_async_remote_copy(
                    part_send.at[where_to],
                    part_recv.at[where_to],
                    part_send_sem,
                    part_recv_sem,
                    device_id=(dp, mp_of(y_off, z_off)),
                    device_id_type=MESH,
                ).start()

            if z_off > 0:
                send()
            else:
                pl.when(step < ny - 1)(send)

                @pl.when(step == ny - 1)
                def _(term=term):
                    own_part[...] = term

        return carry

    lax.fori_loop(0, ny, chunk, 0)

    pooled_tokens = jnp.sum(x_buf[ny - 1, pl.ds(0, rows)].astype(F32), axis=1) * (1.0 / patches)
    tower = pooled_tokens + own_part[...]

    id_blocks = []
    lane_row = lax.broadcasted_iota(jnp.int32, (8, 128), 0)
    for start in range(0, chips * rows, 8):
        block = jnp.zeros((8, 128), jnp.int32)
        for k in range(8):
            chip, r = (start + k) // rows, (start + k) % rows
            entry = text_ids_s[((chip * 2 + core) * width + mp) * rows + r]
            block = jnp.where(lane_row == k, entry, block)
        id_blocks.append(block)
    id_column = jnp.concatenate(id_blocks, axis=0)[:, :group].astype(F32)

    await_bytes(part_recv, part_recv_sem)
    tower += jnp.sum(part_recv[...].astype(F32), axis=0)
    emb_own[mp] = unit_rows(tower).astype(BF16)
    for y_off, z_off in mp_partners:
        pltpu.make_async_remote_copy(
            emb_own.at[mp],
            emb_own.at[mp],
            emb_send_sem,
            emb_recv_sem,
            device_id=(dp, mp_of(y_off, z_off)),
            device_id_type=MESH,
        ).start()

    def flat(blocks_ref, count):
        for k in range(count):
            rows_f32[pl.ds(k * rows, rows), :] = blocks_ref[k].astype(F32)
        return rows_f32[pl.ds(0, count * rows), :].astype(BF16)

    await_bytes(text_all.at[pl.ds(0, chips - 1)], text_recv_sem)
    text_emb = flat(text_all, chips)
    meta_copy.wait_recv()

    def pair_terms(emb, meta):
        cosines = lax.dot_general(
            text_emb, emb, (((1,), (1,)), ((), ())), preferred_element_type=F32
        )
        logits = scale_v[...] * cosines + bias_v[...]
        same = id_column == meta[pl.ds(0, 1), pl.ds(0, group)]
        sign = jnp.where(same, 1.0, -1.0)
        weights = (
            meta[pl.ds(1, 1), pl.ds(0, group)] * -sign * jax.nn.sigmoid(-sign * logits) * scale_v[...]
        )
        return jnp.dot(weights.astype(BF16), emb, preferred_element_type=F32)

    await_bytes(emb_own.at[pl.ds(0, width - 1)], emb_recv_sem)
    pair_copy = pltpu.make_async_remote_copy(
        emb_own, emb_peer, pair_send_sem, pair_recv_sem, device_id=(partner, mp), device_id_type=MESH
    )
    pair_copy.start()
    grads = pair_terms(flat(emb_own, width), meta_own)
    pair_copy.wait_recv()
    grads += pair_terms(flat(emb_peer, width), meta_peer)

    for k in range(chips):
        grad_send[k] = grads[k * rows : (k + 1) * rows].astype(BF16)
    for index, (x_off, z_off) in enumerate(dp_partners):
        target = dp_of(x_off, z_off)
        pltpu.make_async_remote_copy(
            grad_send.at[target // 2],
            grad_recv.at[index],
            grad_send_sem,
            grad_recv_sem,
            device_id=(target, mp),
            device_id_type=MESH,
        ).start()
    own_grad[...] = grad_send[my_chip].astype(F32)

    await_bytes(part_send, part_send_sem)
    await_bytes(emb_own.at[pl.ds(0, width - 1)], emb_send_sem)
    await_bytes(text_all.at[pl.ds(0, chips - 1)], text_send_sem)
    meta_copy.wait_send()
    pair_copy.wait_send()
    await_bytes(grad_send.at[pl.ds(0, chips - 1)], grad_send_sem)
    await_bytes(grad_recv, grad_recv_sem)
    out[...] = own_grad[...] + jnp.sum(grad_recv[...].astype(F32), axis=0)


def fused(geometry, tokens, counts, image_ids, gain, shift, w_up, w_down, text_rows, text_ids, scale, bias):
    nx, nzh, nzl, ny = geometry
    width, chips = nzl * ny, nx * nzh
    rows, d = text_rows.shape
    units = w_up.shape[1]
    patches = tokens.shape[1]
    group = width * rows
    meta_lanes = -(-group // 128) * 128
    dma = pltpu.SemaphoreType.DMA
    return pl.pallas_call(
        functools.partial(kernel, geometry),
        out_shape=jax.ShapeDtypeStruct((rows, d), F32),
        in_specs=[pl.BlockSpec(memory_space=pl.ANY)] * 11,
        out_specs=pl.BlockSpec(memory_space=pltpu.VMEM),
        scratch_shapes=[
            pltpu.VMEM((ny, nzl * rows, patches, d), BF16),
            pltpu.VMEM(counts.shape, jnp.int32),
            pltpu.VMEM(image_ids.shape, jnp.int32),
            pltpu.VMEM(gain.shape, F32),
            pltpu.VMEM(shift.shape, F32),
            pltpu.VMEM(w_up.shape, BF16),
            pltpu.VMEM(w_down.shape, BF16),
            pltpu.VMEM(text_rows.shape, BF16),
            pltpu.SMEM(text_ids.shape, jnp.int32),
            pltpu.VMEM(scale.shape, F32),
            pltpu.VMEM(bias.shape, F32),
            pltpu.VMEM((d, units + 128), BF16),
            pltpu.VMEM((1, units), F32),
            pltpu.VMEM((1, units), F32),
            pltpu.VMEM((width - 1, rows, d), BF16),
            pltpu.VMEM((width - 1, rows, d), BF16),
            pltpu.VMEM((rows, d), F32),
            pltpu.VMEM((width, rows, d), BF16),
            pltpu.VMEM((width, rows, d), BF16),
            pltpu.VMEM((8, meta_lanes), F32),
            pltpu.VMEM((8, meta_lanes), F32),
            pltpu.VMEM((chips, rows, d), BF16),
            pltpu.VMEM((max(width, chips) * rows, d), F32),
            pltpu.VMEM((chips, rows, d), BF16),
            pltpu.VMEM((chips - 1, rows, d), BF16),
            pltpu.VMEM((rows, d), F32),
            dma((10,)),
            dma((ny,)),
        ]
        + [dma] * 12,
        compiler_params=pltpu.CompilerParams(
            collective_id=0, has_side_effects=True, vmem_limit_bytes=60 * 1024 * 1024
        ),
    )(tokens, counts, image_ids, gain, shift, w_up, w_down, text_rows, text_ids, scale, bias)


def local(
    geometry,
    image_tokens,
    image_counts,
    image_ids,
    norm_gain,
    norm_bias,
    up_weight,
    down_weight,
    text_rows,
    text_counts,
    text_ids,
    logit_scale,
    logit_bias,
):
    grads = fused(
        geometry,
        image_tokens,
        image_counts,
        image_ids.reshape(1, -1),
        norm_gain.reshape(1, -1),
        norm_bias.reshape(1, -1),
        up_weight,
        down_weight,
        text_rows,
        text_ids,
        logit_scale.reshape(1, 1),
        logit_bias.reshape(1, 1),
    )
    text_valid = (jnp.arange(text_rows.shape[0], dtype=jnp.int32) < text_counts[0]).astype(F32)
    return grads * text_valid[:, None]


def solution(mesh, geometry=GEOMETRY):
    placed = (
        P("dp", None, None),
        P("dp", None),
        P("dp"),
        P(),
        P(),
        P(None, "mp"),
        P("mp", None),
        P(("dp", "mp"), None),
        P(("dp", "mp")),
        P(),
        P(),
        P(),
    )
    return jax.shard_map(
        functools.partial(local, geometry),
        mesh=mesh,
        in_specs=placed,
        out_specs=P(("dp", "mp"), None),
        check_vma=False,
    )
```

```python
import functools

import jax
import jax.numpy as jnp
from jax import lax
from jax.experimental import pallas as pl
from jax.experimental.pallas import tpu as pltpu
from jax.sharding import PartitionSpec as P

MESH = pl.DeviceIdType.MESH
EPS = 1e-06
F32 = jnp.float32
BF16 = jnp.bfloat16
GEOMETRY = (4, 4, 3, 8)
GELU_A = 0.7978845608028654
GELU_B = GELU_A * 0.044715
PAIR = 2
GREET = 1


def await_bytes(ref, sem):
    pltpu.make_async_copy(ref, ref, sem).wait()


def unit_rows(values):
    return values * lax.rsqrt(jnp.sum(values * values, axis=-1, keepdims=True) + EPS)


def gelu(u):
    half = 0.5 * u
    return half + half * jnp.tanh(u * (GELU_A + GELU_B * (u * u)))


def y_offset(step, ny):
    half = (step + 1) // 2
    return ny // 2 + half * (1 - 2 * (step % 2))


def kernel(
    geometry,
    tokens,
    counts,
    image_ids,
    gain,
    shift,
    w_up,
    w_down,
    text_rows,
    text_ids,
    scale,
    bias,
    out,
    x_buf,
    counts_v,
    ids_v,
    affine_v,
    up_v,
    down_v,
    text_v,
    text_ids_s,
    scale_s,
    bias_s,
    w_aug,
    pooled_v,
    part_send,
    part_recv,
    own_part,
    emb_own,
    emb_peer,
    meta_own,
    meta_peer,
    text_all,
    rows_f32,
    grad_send,
    grad_recv,
    own_grad,
    in_sem,
    x_sem,
    part_send_sem,
    part_recv_sem,
    emb_send_sem,
    emb_recv_sem,
    pair_send_sem,
    pair_recv_sem,
    meta_send_sem,
    meta_recv_sem,
    text_send_sem,
    text_recv_sem,
    grad_send_sem,
    grad_recv_sem,
):
    nx, nzh, nzl, ny = geometry
    width = nzl * ny
    chips = nx * nzh
    rows, d = text_rows.shape
    patches = tokens.shape[1]
    units = w_up.shape[1]
    group = width * rows
    lanes = d // 128
    dp = lax.axis_index("dp")
    mp = lax.axis_index("mp")
    core = dp % 2
    my_x = dp // (2 * nzh)
    my_zh = (dp // 2) % nzh
    my_zl = mp // ny
    my_y = mp % ny
    partner = dp + 1 - 2 * core
    my_chip = dp // 2

    def mp_of(y_off, z_off):
        return ((my_zl + z_off) % nzl) * ny + (my_y + y_off) % ny

    def dp_of(x_off, z_off):
        return (((my_x + x_off) % nx) * nzh + (my_zh + z_off) % nzh) * 2 + core

    mp_partners = [
        (y_off, z_off)
        for y_off in [y_offset(s, ny) for s in range(ny)]
        for z_off in [(z + 1) % nzl for z in range(nzl)]
    ][:-1]
    z_order = sorted(range(nzh), key=lambda o: -min(o, nzh - o))
    x_order = sorted(range(nx), key=lambda o: -min(o, nx - o))
    dp_partners = [(x_off, z_off) for z_off in z_order for x_off in x_order][:-1]

    small = [
        (w_up, up_v),
        (gain, affine_v.at[pl.ds(0, lanes)]),
        (shift, affine_v.at[pl.ds(16, lanes)]),
        (w_down, down_v),
        (text_rows, text_v),
        (counts, counts_v),
        (image_ids, ids_v),
        (text_ids, text_ids_s),
        (scale, scale_s),
        (bias, bias_s),
    ]
    for index, (source, target) in enumerate(small[:3]):
        pltpu.make_async_copy(source, target, in_sem.at[index]).start()

    def load(step, z_off):
        start = mp_of(y_offset(step, ny), z_off) * rows
        pltpu.make_async_copy(
            tokens.at[pl.ds(start, rows)], x_buf.at[step, pl.ds(z_off * rows, rows)], x_sem.at[step]
        ).start()

    def load_step(step):
        for z_off in range(nzl):
            load(step, z_off)

    load_step(0)
    barrier = pltpu.get_barrier_semaphore()
    for y_off, z_off in mp_partners:
        pl.semaphore_signal(barrier, inc=1, device_id=(dp, mp_of(y_off, z_off)), device_id_type=MESH)
    for x_off, z_off in dp_partners:
        pl.semaphore_signal(barrier, inc=1, device_id=(dp_of(x_off, z_off), mp), device_id_type=MESH)
    pl.semaphore_signal(barrier, inc=1, device_id=(partner, mp), device_id_type=MESH)

    for step in range(1, ny):
        load_step(step)
        if step == 1:
            for index, (source, target) in enumerate(small):
                if index >= 3:
                    pltpu.make_async_copy(source, target, in_sem.at[index]).start()
    for index in range(3):
        pltpu.make_async_copy(*small[index], in_sem.at[index]).wait()

    columns = jnp.transpose(affine_v[...])
    total = jnp.zeros((8, units), F32)
    moved = jnp.zeros((8, units), F32)
    for j in range(lanes):
        cut = pl.ds(j * 128, 128)
        block = up_v[cut, :].astype(F32)
        scaled = (block * columns[:, j : j + 1]).astype(BF16)
        w_aug[cut, pl.ds(0, units)] = scaled
        w_aug[cut, pl.ds(units, 128)] = jnp.ones((128, 128), BF16)
        total += jnp.sum(scaled.astype(F32).reshape(16, 8, units), axis=0)
        moved += jnp.sum((block * columns[:, 16 + j : 17 + j]).reshape(16, 8, units), axis=0)
    w_sum = jnp.sum(total, axis=0, keepdims=True)
    w_shift = jnp.sum(moved, axis=0, keepdims=True)

    meta_copy = pltpu.make_async_remote_copy(
        meta_own, meta_peer, meta_send_sem, meta_recv_sem, device_id=(partner, mp), device_id_type=MESH
    )

    def own_rows():
        for index in range(3, len(small)):
            pltpu.make_async_copy(*small[index], in_sem.at[index]).wait()

        text_all[my_chip] = unit_rows(text_v[...].astype(F32)).astype(BF16)
        slot = lax.broadcasted_iota(jnp.int32, (width, group), 1)
        owner = lax.broadcasted_iota(jnp.int32, (width, group), 0)
        spread = jnp.where(slot // rows == owner, 1.0, 0.0).astype(BF16)
        row_counts = jnp.dot(
            jnp.broadcast_to(counts_v[...].astype(F32), (8, width)).astype(BF16),
            spread,
            preferred_element_type=F32,
        )[:1]
        place = (lax.broadcasted_iota(jnp.int32, (1, group), 1) % rows).astype(F32)
        meta_own[pl.ds(0, 1), pl.ds(0, group)] = ids_v[...].astype(F32)
        meta_own[pl.ds(1, 1), pl.ds(0, group)] = jnp.where(place < row_counts, 1.0, 0.0)

    images = nzl * rows
    tokens_of = rows * patches

    def project(step):
        await_bytes(x_buf.at[step], x_sem.at[step])
        return jnp.dot(
            x_buf[step].reshape(images * patches, d), w_aug[...], preferred_element_type=F32
        )

    def pool(step, product):
        for z_off in range(nzl):
            part = product[z_off * tokens_of : (z_off + 1) * tokens_of]
            mean = part[:, units:] * (1.0 / d)
            near = mean.astype(BF16)
            wide = jnp.concatenate([near, near], axis=1)
            squares = jnp.zeros((tokens_of, 128), F32)
            for at in range(0, d, 256):
                size = min(256, d - at)
                piece = x_buf[step, pl.ds(z_off * rows, rows), :, pl.ds(at, size)]
                piece = piece.reshape(tokens_of, size) - wide[:, :size]
                square = (piece * piece).astype(F32)
                squares += square[:, :128]
                if size > 128:
                    squares += square[:, 128:]
            rest = mean[:, :1] - near[:, :1].astype(F32)
            spread_of = jnp.sum(squares, axis=-1, keepdims=True) * (1.0 / d) - rest * rest
            before = (part[:, :units] - mean * w_sum) * lax.rsqrt(spread_of + EPS) + w_shift
            hidden = gelu(before).astype(BF16).astype(F32)
            pooled_v[pl.ds(step * images + z_off * rows, rows), :] = jnp.sum(
                hidden.reshape(rows, patches, units), axis=1
            ) * (1.0 / patches)

    def slot_of(step, z_off):
        return step * nzl + (z_off + nzl - 1) % nzl

    def send(step):
        for z_off in [(z + 1) % nzl for z in range(nzl)]:
            if (step, z_off) != (ny - 1, 0):
                pltpu.make_async_remote_copy(
                    part_send.at[slot_of(step, z_off)],
                    part_recv.at[slot_of(step, z_off)],
                    part_send_sem,
                    part_recv_sem,
                    device_id=(dp, mp_of(y_offset(step, ny), z_off)),
                    device_id_type=MESH,
                ).start()

    product = project(0)
    for step in range(ny):
        following = project(step + 1) if step + 1 < ny else None
        pool(step, product)
        product = following
        if step % PAIR == PAIR - 1:
            first = step - PAIR + 1
            if first == 0:
                own_rows()
            part = jnp.dot(
                pooled_v[pl.ds(first * images, PAIR * images), :].astype(BF16),
                down_v[...],
                preferred_element_type=F32,
            )
            for done in range(first, step + 1):
                for z_off in range(nzl):
                    at = (done - first) * images + z_off * rows
                    term = part[at : at + rows]
                    if (done, z_off) == (ny - 1, 0):
                        own_part[...] = term
                    else:
                        part_send[slot_of(done, z_off)] = term.astype(BF16)
            ready = step // PAIR + 1
            if ready == GREET:
                pl.semaphore_wait(barrier, len(mp_partners) + len(dp_partners) + 1)
            if ready >= GREET:
                for done in range(0 if ready == GREET else first, step + 1):
                    send(done)
            if ready == GREET:
                meta_copy.start()
                for z_off in z_order[:-1]:
                    pltpu.make_async_remote_copy(
                        text_all.at[my_chip],
                        text_all.at[my_chip],
                        text_send_sem.at[0],
                        text_recv_sem.at[0],
                        device_id=(dp_of(0, z_off), mp),
                        device_id_type=MESH,
                    ).start()

    await_bytes(text_all.at[pl.ds(0, nzh - 1)], text_recv_sem.at[0])
    text_mine = text_all.at[pl.ds(my_x * nzh, nzh)]
    for x_off in x_order[:-1]:
        pltpu.make_async_remote_copy(
            text_mine,
            text_mine,
            text_send_sem.at[1],
            text_recv_sem.at[1],
            device_id=(dp_of(x_off, 0), mp),
            device_id_type=MESH,
        ).start()

    pooled_tokens = jnp.sum(x_buf[ny - 1, pl.ds(0, rows)].astype(F32), axis=1) * (1.0 / patches)
    tower = pooled_tokens + own_part[...]

    id_blocks = []
    lane_row = lax.broadcasted_iota(jnp.int32, (8, 128), 0)
    for start in range(0, chips * rows, 8):
        block = jnp.zeros((8, 128), jnp.int32)
        for k in range(8):
            chip, r = (start + k) // rows, (start + k) % rows
            entry = text_ids_s[((chip * 2 + core) * width + mp) * rows + r]
            block = jnp.where(lane_row == k, entry, block)
        id_blocks.append(block)
    id_column = jnp.concatenate(id_blocks, axis=0)[:, :group].astype(F32)

    await_bytes(part_recv, part_recv_sem)
    tower += jnp.sum(part_recv[...].astype(F32), axis=0)
    emb_own[mp] = unit_rows(tower).astype(BF16)
    for y_off, z_off in mp_partners:
        pltpu.make_async_remote_copy(
            emb_own.at[mp],
            emb_own.at[mp],
            emb_send_sem,
            emb_recv_sem,
            device_id=(dp, mp_of(y_off, z_off)),
            device_id_type=MESH,
        ).start()

    def flat(blocks_ref, count):
        for k in range(count):
            rows_f32[pl.ds(k * rows, rows), :] = blocks_ref[k].astype(F32)
        return rows_f32[pl.ds(0, count * rows), :].astype(BF16)

    if nx > 1:
        await_bytes(text_all.at[pl.ds(0, chips - nzh)], text_recv_sem.at[1])
    text_emb = flat(text_all, chips)
    meta_copy.wait_recv()

    def pair_terms(emb, meta):
        cosines = lax.dot_general(
            text_emb, emb, (((1,), (1,)), ((), ())), preferred_element_type=F32
        )
        logits = scale_s[0] * cosines + bias_s[0]
        same = id_column == meta[pl.ds(0, 1), pl.ds(0, group)]
        sign = jnp.where(same, 1.0, -1.0)
        weights = (
            meta[pl.ds(1, 1), pl.ds(0, group)] * -sign * jax.nn.sigmoid(-sign * logits) * scale_s[0]
        )
        return jnp.dot(weights.astype(BF16), emb, preferred_element_type=F32)

    await_bytes(emb_own.at[pl.ds(0, width - 1)], emb_recv_sem)
    pair_copy = pltpu.make_async_remote_copy(
        emb_own, emb_peer, pair_send_sem, pair_recv_sem, device_id=(partner, mp), device_id_type=MESH
    )
    pair_copy.start()
    grads = pair_terms(flat(emb_own, width), meta_own)
    pair_copy.wait_recv()
    grads += pair_terms(flat(emb_peer, width), meta_peer)

    for k in range(chips):
        grad_send[k] = grads[k * rows : (k + 1) * rows].astype(BF16)
    for index, (x_off, z_off) in enumerate(dp_partners):
        target = dp_of(x_off, z_off)
        pltpu.make_async_remote_copy(
            grad_send.at[target // 2],
            grad_recv.at[index],
            grad_send_sem,
            grad_recv_sem,
            device_id=(target, mp),
            device_id_type=MESH,
        ).start()
    own_grad[...] = grad_send[my_chip].astype(F32)

    await_bytes(part_send, part_send_sem)
    await_bytes(emb_own.at[pl.ds(0, width - 1)], emb_send_sem)
    await_bytes(text_all.at[pl.ds(0, nzh - 1)], text_send_sem.at[0])
    if nx > 1:
        await_bytes(text_all.at[pl.ds(0, chips - nzh)], text_send_sem.at[1])
    meta_copy.wait_send()
    pair_copy.wait_send()
    await_bytes(grad_send.at[pl.ds(0, chips - 1)], grad_send_sem)
    await_bytes(grad_recv, grad_recv_sem)
    out[...] = own_grad[...] + jnp.sum(grad_recv[...].astype(F32), axis=0)


def fused(geometry, tokens, counts, image_ids, gain, shift, w_up, w_down, text_rows, text_ids, scale, bias):
    nx, nzh, nzl, ny = geometry
    width, chips = nzl * ny, nx * nzh
    rows, d = text_rows.shape
    units = w_up.shape[1]
    patches = tokens.shape[1]
    group = width * rows
    meta_lanes = -(-group // 128) * 128
    dma = pltpu.SemaphoreType.DMA
    return pl.pallas_call(
        functools.partial(kernel, geometry),
        out_shape=pltpu.VMEM((rows, d), F32),
        in_specs=[pl.BlockSpec(memory_space=pltpu.HBM)] * 11,
        out_specs=pl.BlockSpec(memory_space=pltpu.VMEM),
        scratch_shapes=[
            pltpu.VMEM((ny, nzl * rows, patches, d), BF16),
            pltpu.VMEM(counts.shape, jnp.int32),
            pltpu.VMEM(image_ids.shape, jnp.int32),
            pltpu.VMEM((32, 128), F32),
            pltpu.VMEM(w_up.shape, BF16),
            pltpu.VMEM(w_down.shape, BF16),
            pltpu.VMEM(text_rows.shape, BF16),
            pltpu.SMEM(text_ids.shape, jnp.int32),
            pltpu.SMEM(scale.shape, F32),
            pltpu.SMEM(bias.shape, F32),
            pltpu.VMEM((d, units + 128), BF16),
            pltpu.VMEM((group, units), F32),
            pltpu.VMEM((width - 1, rows, d), BF16),
            pltpu.VMEM((width - 1, rows, d), BF16),
            pltpu.VMEM((rows, d), F32),
            pltpu.VMEM((width, rows, d), BF16),
            pltpu.VMEM((width, rows, d), BF16),
            pltpu.VMEM((8, meta_lanes), F32),
            pltpu.VMEM((8, meta_lanes), F32),
            pltpu.VMEM((chips, rows, d), BF16),
            pltpu.VMEM((max(width, chips) * rows, d), F32),
            pltpu.VMEM((chips, rows, d), BF16),
            pltpu.VMEM((chips - 1, rows, d), BF16),
            pltpu.VMEM((rows, d), F32),
            dma((10,)),
            dma((ny,)),
        ]
        + [dma] * 8
        + [dma((2,)), dma((2,)), dma, dma],
        compiler_params=pltpu.CompilerParams(
            collective_id=0, has_side_effects=True, vmem_limit_bytes=60 * 1024 * 1024
        ),
    )(tokens, counts, image_ids, gain, shift, w_up, w_down, text_rows, text_ids, scale, bias)


def local(
    geometry,
    image_tokens,
    image_counts,
    image_ids,
    norm_gain,
    norm_bias,
    up_weight,
    down_weight,
    text_rows,
    text_counts,
    text_ids,
    logit_scale,
    logit_bias,
):
    grads = fused(
        geometry,
        image_tokens,
        image_counts,
        image_ids.reshape(1, -1),
        norm_gain.reshape(-1, 128),
        norm_bias.reshape(-1, 128),
        up_weight,
        down_weight,
        text_rows,
        text_ids,
        logit_scale,
        logit_bias,
    )
    text_valid = (jnp.arange(text_rows.shape[0], dtype=jnp.int32) < text_counts[0]).astype(F32)
    return grads * text_valid[:, None]


def solution(mesh, geometry=GEOMETRY):
    placed = (
        P("dp", None, None),
        P("dp", None),
        P("dp"),
        P(),
        P(),
        P(None, "mp"),
        P("mp", None),
        P(("dp", "mp"), None),
        P(("dp", "mp")),
        P(),
        P(),
        P(),
    )
    return jax.shard_map(
        functools.partial(local, geometry),
        mesh=mesh,
        in_specs=placed,
        out_specs=P(("dp", "mp"), None),
        check_vma=False,
    )
```
